32 devices in a mesh: eq: 2 (over x), row: 4 (over y, core), col: 4 (over z).
Axes of the slice: x: 2, y: 2, z: 4, core: 2. Of those that a mesh axis runs over, the one named last changes fastest.
Arguments:
- transition: float32 [6144, 3072], P(('eq', 'row'), 'col'), parts along dimension 0, may hold values from -0.05 to 0.9
- covariance: float32 [6144, 3072], P(('eq', 'row'), 'col'), parts along dimension 0, may hold values from -1 to 5, as said below
Outputs:
- covariance_out: float32 [6144, 3072], P(('eq', 'row'), 'col'), parts along dimension 0
- transition_out: float32 [6144, 3072], P(('eq', 'row'), 'col'), parts along dimension 0
The draws below stay inside these ranges and needn't reach their ends.
There are 2 independent parts, one for each index of `eq`. The reference program is written for one: setup_inputs(seed, part) draws one part's arguments, and reference() takes and returns one part's arrays. A program takes and returns all parts, laid end to end along the dimension named above; each array names one. Nothing has to cross between parts.
Inputs may be any that keep to these rules, and one draw needn't show every extreme that they name: covariance is exactly symmetric.
All inputs are finite; a program needn't handle non-finite values.
Results may differ from the reference program's by a relative error of at most 0.0001.
Values sent between devices are 32-bit elements; how exact they have to be, the bound alone decides.
A program may use at most 128 MiB of HBM per device.

```python
import jax
import jax.numpy as jnp
from jax import lax

ORDER = 3072
STEPS = 1


def draw_transition(key, part):
    keys = jax.random.split(jax.random.fold_in(key, 11), 2)
    diagonal = jax.random.uniform(keys[0], (ORDER,), jnp.float32, 0.5, 0.85)
    noise = jnp.clip(jax.random.normal(keys[1], (ORDER, ORDER), jnp.float32), -6.0, 6.0) * (0.12 / ORDER ** 0.5)
    noise = jnp.clip(noise, -0.05, 0.05)
    return noise + jnp.diag(diagonal)


def draw_covariance(key, part):
    keys = jax.random.split(jax.random.fold_in(key, 23), 3)
    diagonal = jax.random.uniform(keys[0], (ORDER,), jnp.float32, 1.0, 3.0)
    normals = jnp.clip(jax.random.normal(keys[1], (ORDER, ORDER), jnp.float32), -6.0, 6.0)
    noise = jnp.clip(normals * (0.4 / (2.0 * ORDER) ** 0.5), -0.45, 0.45)
    result = noise + noise.T + jnp.diag(diagonal)
    return result


def setup_inputs(seed: int = 0, part: int = 0) -> dict:
    key_list = jax.random.split(jax.random.key(seed), 3)
    part_splits = jax.random.split(jax.random.fold_in(key_list[2], part), 3)
    transition = draw_transition(jax.random.fold_in(jax.random.fold_in(key_list[2], part), 71), part)
    covariance = draw_covariance(jax.random.fold_in(jax.random.fold_in(key_list[2], part), 71), part)
    return dict(transition=transition, covariance=covariance)


def reference(transition, covariance):
    highest = lax.Precision.HIGHEST
    matrix = transition
    current = covariance
    for repeat in range(STEPS):
        product = jnp.dot(matrix, current, precision=highest, preferred_element_type=jnp.float32)
        current = jnp.dot(product, matrix.T, precision=highest, preferred_element_type=jnp.float32) + current
        matrix = jnp.dot(matrix, matrix, precision=highest, preferred_element_type=jnp.float32)
    return current, matrix
```

```python
import functools

import jax
import jax.numpy as jnp
from jax import lax
from jax.sharding import PartitionSpec as P

CHUNKS = 4


def dot(left, right, transposed=False):
    return lax.dot_general(
        left,
        right,
        (((1,), (1 if transposed else 0,)), ((), ())),
        precision=lax.Precision.HIGH,
        preferred_element_type=jnp.float32,
    )


def shift(block, senders, step):
    return lax.ppermute(block, "col", [(z, z + step) for z in senders])


def gather_column(block, count, place):
    me = lax.axis_index("row")
    size = block.shape[0]
    held = {0: block}
    stride = count // 2
    while stride:
        pairs = [(i, i ^ stride) for i in range(count)]
        for key in list(held):
            held[key ^ stride] = lax.ppermute(held[key], "row", pairs)
        stride //= 2
    whole = jnp.zeros((count * size, block.shape[1]), block.dtype)
    for key, value in held.items():
        where = lax.rem((me ^ key) - place + count, count) * size
        whole = lax.dynamic_update_slice(whole, value, (where, 0))
    return whole


def per_device(count, transition, covariance):
    place = lax.axis_index("col")
    rows, width = transition.shape
    step = rows // CHUNKS

    def gather_rows(piece):
        left, right = {0: piece}, {0: piece}
        for s in range(1, count):
            left[s] = shift(left[s - 1], range(1, count - s + 1), -1)
            right[s] = shift(right[s - 1], range(s - 1, count - 1), 1)
        slots = [piece]
        for s in range(1, count):
            slots.append(jnp.where(place + s < count, left[s], right[count - s]))
        return jnp.concatenate(slots, axis=1)

    def reduce_rows(partial):
        slots = [partial[:, s * width : (s + 1) * width] for s in range(count)]
        to_left = to_right = None
        for s in range(count - 1, 0, -1):
            a = slots[count - s] if to_left is None else to_left + slots[count - s]
            b = slots[s] if to_right is None else to_right + slots[s]
            to_left = shift(a, range(s, count), -1)
            to_right = shift(b, range(0, count - s), 1)
        return slots[0] + (to_left + to_right)

    pieces = [gather_rows(transition[c * step : (c + 1) * step]) for c in range(CHUNKS)]
    covariance_column = gather_column(covariance, count, place)
    transition_column = gather_column(transition, count, place)
    updates, squares = [], []
    for piece in pieces:
        product = dot(piece, covariance_column)
        updates.append(reduce_rows(dot(product, transition_column, transposed=True)))
        squares.append(dot(piece, transition_column))
    return jnp.concatenate(updates, axis=0) + covariance, jnp.concatenate(squares, axis=0)


def solution(mesh):
    count = mesh.shape["col"]
    assert mesh.shape["row"] == count
    spec = P(("eq", "row"), "col")
    return jax.shard_map(
        functools.partial(per_device, count),
        mesh=mesh,
        in_specs=(spec, spec),
        out_specs=(spec, spec),
        check_vma=False,
    )
```

```python
import functools

import jax
import jax.numpy as jnp
from jax import lax
from jax.experimental import pallas as pl
from jax.experimental.pallas import tpu as pltpu
from jax.sharding import PartitionSpec as P

CHUNKS = 4
TILE = 256
LEFT, RIGHT = 0, 1


def split(value):
    high = value.astype(jnp.bfloat16)
    return high, (value - high.astype(jnp.float32)).astype(jnp.bfloat16)


def product(left, right, transposed=False):
    dims = (((1,), (1 if transposed else 0,)), ((), ()))
    dot = functools.partial(lax.dot_general, dimension_numbers=dims, preferred_element_type=jnp.float32)
    return dot(left[0], right[0]) + (dot(left[0], right[1]) + dot(left[1], right[0]))


def kernel(
    n, a_ref, x_ref, update_ref, square_ref,
    a_row, a_col, x_col, partial, arrived, y_high, y_low,
    local_sems, row_send, row_recv, gather_send, gather_recv, reduce_send, reduce_recv,
):
    r, z = lax.axis_index("row"), lax.axis_index("col")
    size = a_ref.shape[0]
    step = size // CHUNKS
    far = lax.rem(r + n // 2, n)
    near = r + 1 - 2 * lax.rem(r, 2)

    def block_of(m):
        base = jnp.where(lax.rem(m, 2) == 0, r, near)
        return lax.rem(base + (m // 2) * 2, n)

    def rows(c):
        return pl.ds(c * step, step)

    local = [
        pltpu.make_async_copy(a_ref, a_row.at[z], local_sems.at[0]),
        pltpu.make_async_copy(a_ref, a_col.at[r], local_sems.at[1]),
        pltpu.make_async_copy(x_ref, x_col.at[r], local_sems.at[2]),
    ]
    for copy in local:
        copy.start()

    barrier = pltpu.get_barrier_semaphore()
    pl.semaphore_signal(barrier, inc=1, device_id={"row": far}, device_id_type=pl.DeviceIdType.MESH)
    pl.semaphore_signal(barrier, inc=1, device_id={"row": near}, device_id_type=pl.DeviceIdType.MESH)

    @pl.when(z > 0)
    def _():
        pl.semaphore_signal(barrier, inc=1, device_id={"col": z - 1}, device_id_type=pl.DeviceIdType.MESH)

    @pl.when(z < n - 1)
    def _():
        pl.semaphore_signal(barrier, inc=1, device_id={"col": z + 1}, device_id_type=pl.DeviceIdType.MESH)

    pl.semaphore_wait(barrier, 4 - jnp.where(z == 0, 1, 0) - jnp.where(z == n - 1, 1, 0))

    for copy in local:
        copy.wait()

    def row_copy(which, kind):
        buffer = (x_col, a_col)[which]
        block = far if kind == 2 else r
        return pltpu.make_async_remote_copy(
            src_ref=buffer.at[block],
            dst_ref=buffer.at[block],
            send_sem=row_send.at[which, kind],
            recv_sem=row_recv.at[which, kind],
            device_id={"row": far if kind == 0 else near},
            device_id_type=pl.DeviceIdType.MESH,
        )

    def row_wait(which, kind):
        buffer = (x_col, a_col)[which]
        block = (far, near, lax.rem(near + n // 2, n))[kind]
        pltpu.make_async_remote_copy(
            src_ref=buffer.at[block],
            dst_ref=buffer.at[block],
            send_sem=row_send.at[which, kind],
            recv_sem=row_recv.at[which, kind],
            device_id={"row": near},
            device_id_type=pl.DeviceIdType.MESH,
        ).wait_recv()

    def gather_copy(side, hop, c, block, target):
        return pltpu.make_async_remote_copy(
            src_ref=a_row.at[block, rows(c)],
            dst_ref=a_row.at[block, rows(c)],
            send_sem=gather_send.at[side, hop, c],
            recv_sem=gather_recv.at[side, hop, c],
            device_id={"col": target},
            device_id_type=pl.DeviceIdType.MESH,
        )

    def gather_each(hop, c, act):
        @pl.when((z > 0) & (z + hop <= n - 1))
        def _():
            act(gather_copy(LEFT, hop, c, z + hop, z - 1))

        @pl.when((z < n - 1) & (z - hop >= 0))
        def _():
            act(gather_copy(RIGHT, hop, c, z - hop, z + 1))

    def gather_send_hop(hop, c):
        gather_each(hop, c, lambda copy: copy.start())

    def gather_wait(hop, c):
        @pl.when(z + 1 + hop <= n - 1)
        def _():
            gather_copy(LEFT, hop, c, z + 1 + hop, z + 1).wait_recv()

        @pl.when(z - 1 - hop >= 0)
        def _():
            gather_copy(RIGHT, hop, c, z - 1 - hop, z - 1).wait_recv()

    def forward(hop, c):
        gather_wait(hop, c)
        gather_send_hop(hop + 1, c)

    def multiply(c, column, store):
        def tile(t, carry):
            lanes = pl.ds(pl.multiple_of(t * TILE, TILE), TILE)

            def one(k, total):
                return total + product(split(a_row[k, rows(c)]), split(column[k, :, lanes]))

            store(lanes, lax.fori_loop(0, n, one, jnp.zeros((step, TILE), jnp.float32)))
            return carry

        lax.fori_loop(0, size // TILE, tile, 0)

    def compute_y(c):
        def store(lanes, value):
            high, low = split(value)
            y_high[rows(c), lanes] = high
            y_low[rows(c), lanes] = low

        multiply(c, x_col, store)

    def compute_square(c):
        def store(lanes, value):
            square_ref[rows(c), lanes] = value

        multiply(c, a_col, store)

    def reduce_copy(side, d, m, c):
        slot = d if side == LEFT else jnp.where(d == z + 1, n, d)
        return pltpu.make_async_remote_copy(
            src_ref=partial.at[d, rows(c)],
            dst_ref=arrived.at[slot, rows(c)],
            send_sem=reduce_send.at[m, c],
            recv_sem=reduce_recv.at[slot, c],
            device_id={"col": z - 1 if side == LEFT else z + 1},
            device_id_type=pl.DeviceIdType.MESH,
        )

    def reduce_wait(slot, c):
        pltpu.make_async_remote_copy(
            src_ref=arrived.at[slot, rows(c)],
            dst_ref=arrived.at[slot, rows(c)],
            send_sem=reduce_send.at[0, c],
            recv_sem=reduce_recv.at[slot, c],
            device_id={"row": near},
            device_id_type=pl.DeviceIdType.MESH,
        ).wait_recv()

    def start_partials(c, low, high):
        per = size // TILE

        def tile(i, carry):
            d = block_of(i // per)
            lanes = pl.ds(pl.multiple_of(lax.rem(i, per) * TILE, TILE), TILE)
            partial[d, rows(c), lanes] = product(
                (y_high[rows(c)], y_low[rows(c)]), split(a_col[d, lanes]), transposed=True
            )
            return carry

        lax.fori_loop(low * per, high * per, tile, 0)

        def send(m, carry):
            d = block_of(m)

            @pl.when((z == n - 1) & (d < z))
            def _():
                reduce_copy(LEFT, d, m, c).start()

            @pl.when((z == 0) & (d > z))
            def _():
                reduce_copy(RIGHT, d, m, c).start()

            return carry

        lax.fori_loop(low, high, send, 0)

    def pass_on(hop, c, low, high):
        def one(m, carry):
            d = block_of(m)

            def add():
                reduce_wait(d, c)
                partial[d, rows(c)] = partial[d, rows(c)] + arrived[d, rows(c)]

            @pl.when((z == n - 1 - hop) & (d < z))
            def _():
                add()
                reduce_copy(LEFT, d, m, c).start()

            @pl.when((z == hop) & (d > z))
            def _():
                add()
                reduce_copy(RIGHT, d, m, c).start()

            return carry

        lax.fori_loop(low, high, one, 0)

    def finish(c):
        update_ref[rows(c)] = x_col[r, rows(c)] + partial[z, rows(c)]

        @pl.when(z < n - 1)
        def _():
            reduce_wait(z, c)
            update_ref[rows(c)] = update_ref[rows(c)] + arrived[z, rows(c)]

        @pl.when(z > 0)
        def _():
            reduce_wait(n, c)
            update_ref[rows(c)] = update_ref[rows(c)] + arrived[n, rows(c)]

    half = n // 2
    gather_send_hop(0, 0)
    for which in range(2):
        row_copy(which, 0).start()
        row_copy(which, 1).start()
    forward(0, 0)
    forward(1, 0)
    gather_send_hop(0, 1)
    forward(0, 1)
    row_wait(0, 0)
    row_copy(0, 2).start()
    forward(1, 1)
    gather_send_hop(0, 2)
    row_wait(0, 1)
    row_wait(0, 2)
    row_wait(1, 1)
    gather_wait(2, 0)
    compute_y(0)
    start_partials(0, 0, half)
    forward(0, 2)
    pass_on(1, 0, 0, half)
    forward(1, 2)
    gather_send_hop(0, 3)
    gather_wait(2, 1)
    compute_y(1)
    start_partials(1, 0, half)
    pass_on(2, 0, 0, half)
    row_wait(1, 0)
    row_copy(1, 2).start()
    pass_on(1, 1, 0, half)
    row_wait(1, 2)
    start_partials(0, half, n)
    start_partials(1, half, n)
    forward(0, 3)
    pass_on(2, 1, 0, half)
    pass_on(1, 0, half, n)
    forward(1, 3)
    pass_on(1, 1, half, n)
    gather_wait(2, 2)
    compute_y(2)
    start_partials(2, 0, n)
    pass_on(2, 0, half, n)
    pass_on(2, 1, half, n)
    compute_square(0)
    pass_on(1, 2, 0, n)
    gather_wait(2, 3)
    compute_y(3)
    start_partials(3, 0, n)
    pass_on(2, 2, 0, n)
    compute_square(1)
    pass_on(1, 3, 0, n)
    compute_square(2)
    pass_on(2, 3, 0, n)
    compute_square(3)
    for c in range(CHUNKS):
        finish(c)

    for which in range(2):
        for kind in range(3):
            row_copy(which, kind).wait_send()
    for c in range(CHUNKS):
        for hop in range(n - 1):
            gather_each(hop, c, lambda copy: copy.wait_send())

        def wait_sent(m, carry):
            d = block_of(m)

            @pl.when(d != z)
            def _():
                reduce_copy(LEFT, d, m, c).wait_send()

            return carry

        lax.fori_loop(0, n, wait_sent, 0)


def per_device(n, transition, covariance):
    size = transition.shape[0]
    f32 = jnp.float32
    shape = jax.ShapeDtypeStruct(transition.shape, f32)
    return pl.pallas_call(
        functools.partial(kernel, n),
        out_shape=(shape, shape),
        in_specs=[pl.BlockSpec(memory_space=pl.ANY)] * 2,
        out_specs=(pl.BlockSpec(memory_space=pltpu.VMEM),) * 2,
        scratch_shapes=[
            pltpu.VMEM((n, size, size), f32),
            pltpu.VMEM((n, size, size), f32),
            pltpu.VMEM((n, size, size), f32),
            pltpu.VMEM((n, size, size), f32),
            pltpu.VMEM((n + 1, size, size), f32),
            pltpu.VMEM((size, size), jnp.bfloat16),
            pltpu.VMEM((size, size), jnp.bfloat16),
            pltpu.SemaphoreType.DMA((3,)),
            pltpu.SemaphoreType.DMA((2, 3)),
            pltpu.SemaphoreType.DMA((2, 3)),
            pltpu.SemaphoreType.DMA((2, n - 1, CHUNKS)),
            pltpu.SemaphoreType.DMA((2, n - 1, CHUNKS)),
            pltpu.SemaphoreType.DMA((n, CHUNKS)),
            pltpu.SemaphoreType.DMA((n + 1, CHUNKS)),
        ],
        compiler_params=pltpu.CompilerParams(
            collective_id=0, has_side_effects=True, vmem_limit_bytes=67043328
        ),
    )(transition, covariance)


def solution(mesh):
    n = mesh.shape["col"]
    assert mesh.shape["row"] == n == 4
    spec = P(("eq", "row"), "col")
    return jax.shard_map(
        functools.partial(per_device, n),
        mesh=mesh,
        in_specs=(spec, spec),
        out_specs=(spec, spec),
        check_vma=False,
    )
```

```python
import functools

import jax
import jax.numpy as jnp
from jax import lax
from jax.experimental import pallas as pl
from jax.experimental.pallas import tpu as pltpu
from jax.sharding import PartitionSpec as P

CHUNKS = 4
TILE = 256
LEFT, RIGHT = 0, 1


def split(value):
    high = value.astype(jnp.bfloat16)
    return high, (value - high.astype(jnp.float32)).astype(jnp.bfloat16)


def product(left, right, transposed=False):
    dims = (((1,), (1 if transposed else 0,)), ((), ()))
    dot = functools.partial(lax.dot_general, dimension_numbers=dims, preferred_element_type=jnp.float32)
    return dot(left[0], right[0]) + (dot(left[0], right[1]) + dot(left[1], right[0]))


def kernel(
    n, a_ref, x_ref, update_ref, square_ref,
    a_row, a_col, x_col, partial, arrived, y_high, y_low,
    local_sems, row_send, row_recv, gather_send, gather_recv, reduce_send, reduce_recv,
):
    r, z = lax.axis_index("row"), lax.axis_index("col")
    size = a_ref.shape[0]
    step = size // CHUNKS
    far = lax.rem(r + n // 2, n)
    near = r + 1 - 2 * lax.rem(r, 2)

    def block_of(m):
        base = jnp.where(lax.rem(m, 2) == 0, r, near)
        return lax.rem(base + (m // 2) * 2, n)

    def rows(c):
        return pl.ds(c * step, step)

    local = [
        pltpu.make_async_copy(a_ref, a_row.at[z], local_sems.at[0]),
        pltpu.make_async_copy(a_ref, a_col.at[r], local_sems.at[1]),
        pltpu.make_async_copy(x_ref, x_col.at[r], local_sems.at[2]),
    ]
    for copy in local:
        copy.start()

    barrier = pltpu.get_barrier_semaphore()
    pl.semaphore_signal(barrier, inc=1, device_id={"row": far}, device_id_type=pl.DeviceIdType.MESH)
    pl.semaphore_signal(barrier, inc=1, device_id={"row": near}, device_id_type=pl.DeviceIdType.MESH)

    @pl.when(z > 0)
    def _():
        pl.semaphore_signal(barrier, inc=1, device_id={"col": z - 1}, device_id_type=pl.DeviceIdType.MESH)

    @pl.when(z < n - 1)
    def _():
        pl.semaphore_signal(barrier, inc=1, device_id={"col": z + 1}, device_id_type=pl.DeviceIdType.MESH)

    pl.semaphore_wait(barrier, 4 - jnp.where(z == 0, 1, 0) - jnp.where(z == n - 1, 1, 0))

    for copy in local:
        copy.wait()

    def row_copy(which, kind):
        buffer = (x_col, a_col)[which]
        block = far if kind == 2 else r
        return pltpu.make_async_remote_copy(
            src_ref=buffer.at[block],
            dst_ref=buffer.at[block],
            send_sem=row_send.at[which, kind],
            recv_sem=row_recv.at[which, kind],
            device_id={"row": far if kind == 0 else near},
            device_id_type=pl.DeviceIdType.MESH,
        )

    def row_wait(which, kind):
        buffer = (x_col, a_col)[which]
        block = (far, near, lax.rem(near + n // 2, n))[kind]
        pltpu.make_async_remote_copy(
            src_ref=buffer.at[block],
            dst_ref=buffer.at[block],
            send_sem=row_send.at[which, kind],
            recv_sem=row_recv.at[which, kind],
            device_id={"row": near},
            device_id_type=pl.DeviceIdType.MESH,
        ).wait_recv()

    def gather_copy(side, hop, c, block, target):
        return pltpu.make_async_remote_copy(
            src_ref=a_row.at[block, rows(c)],
            dst_ref=a_row.at[block, rows(c)],
            send_sem=gather_send.at[side, hop, c],
            recv_sem=gather_recv.at[side, hop, c],
            device_id={"col": target},
            device_id_type=pl.DeviceIdType.MESH,
        )

    def gather_each(hop, c, act):
        @pl.when((z > 0) & (z + hop <= n - 1))
        def _():
            act(gather_copy(LEFT, hop, c, z + hop, z - 1))

        @pl.when((z < n - 1) & (z - hop >= 0))
        def _():
            act(gather_copy(RIGHT, hop, c, z - hop, z + 1))

    def gather_send_hop(hop, c):
        gather_each(hop, c, lambda copy: copy.start())

    def gather_wait(hop, c):
        @pl.when(z + 1 + hop <= n - 1)
        def _():
            gather_copy(LEFT, hop, c, z + 1 + hop, z + 1).wait_recv()

        @pl.when(z - 1 - hop >= 0)
        def _():
            gather_copy(RIGHT, hop, c, z - 1 - hop, z - 1).wait_recv()

    def forward(hop, c):
        gather_wait(hop, c)
        gather_send_hop(hop + 1, c)

    def multiply(c, column, store):
        def tile(t, carry):
            lanes = pl.ds(pl.multiple_of(t * TILE, TILE), TILE)

            def one(k, total):
                return total + product(split(a_row[k, rows(c)]), split(column[k, :, lanes]))

            store(lanes, lax.fori_loop(0, n, one, jnp.zeros((step, TILE), jnp.float32)))
            return carry

        lax.fori_loop(0, size // TILE, tile, 0)

    def compute_y(c):
        def store(lanes, value):
            high, low = split(value)
            y_high[rows(c), lanes] = high
            y_low[rows(c), lanes] = low

        multiply(c, x_col, store)

    def compute_square(c):
        def store(lanes, value):
            square_ref[rows(c), lanes] = value

        multiply(c, a_col, store)

    def reduce_copy(side, d, m, c):
        slot = d if side == LEFT else jnp.where(d == z + 1, n, d)
        return pltpu.make_async_remote_copy(
            src_ref=partial.at[d, rows(c)],
            dst_ref=arrived.at[slot, rows(c)],
            send_sem=reduce_send.at[m, c],
            recv_sem=reduce_recv.at[slot, c],
            device_id={"col": z - 1 if side == LEFT else z + 1},
            device_id_type=pl.DeviceIdType.MESH,
        )

    def reduce_wait(slot, c):
        pltpu.make_async_remote_copy(
            src_ref=arrived.at[slot, rows(c)],
            dst_ref=arrived.at[slot, rows(c)],
            send_sem=reduce_send.at[0, c],
            recv_sem=reduce_recv.at[slot, c],
            device_id={"row": near},
            device_id_type=pl.DeviceIdType.MESH,
        ).wait_recv()

    def far_first(i, low, high):
        base = 0 if high - low == n else (block_of(low) // 2) * 2
        return base + i, base + high - low - 1 - i

    def start_partials(c, low, high):
        per = size // TILE

        def tile(i, carry):
            d = block_of(i // per)
            lanes = pl.ds(pl.multiple_of(lax.rem(i, per) * TILE, TILE), TILE)
            partial[d, rows(c), lanes] = product(
                (y_high[rows(c)], y_low[rows(c)]), split(a_col[d, lanes]), transposed=True
            )
            return carry

        lax.fori_loop(low * per, high * per, tile, 0)

        def send(i, carry):
            to_left, to_right = far_first(i, low, high)

            @pl.when((z == n - 1) & (to_left < z))
            def _():
                reduce_copy(LEFT, to_left, to_left, c).start()

            @pl.when((z == 0) & (to_right > z))
            def _():
                reduce_copy(RIGHT, to_right, to_right, c).start()

            return carry

        lax.fori_loop(0, high - low, send, 0)

    def pass_on(hop, c, low, high):
        def one(i, carry):
            to_left, to_right = far_first(i, low, high)

            def add(d):
                reduce_wait(d, c)
                partial[d, rows(c)] = partial[d, rows(c)] + arrived[d, rows(c)]

            @pl.when((z == n - 1 - hop) & (to_left < z))
            def _():
                add(to_left)
                reduce_copy(LEFT, to_left, to_left, c).start()

            @pl.when((z == hop) & (to_right > z))
            def _():
                add(to_right)
                reduce_copy(RIGHT, to_right, to_right, c).start()

            return carry

        lax.fori_loop(0, high - low, one, 0)

    def finish(c):
        update_ref[rows(c)] = x_col[r, rows(c)] + partial[z, rows(c)]

        @pl.when(z < n - 1)
        def _():
            reduce_wait(z, c)
            update_ref[rows(c)] = update_ref[rows(c)] + arrived[z, rows(c)]

        @pl.when(z > 0)
        def _():
            reduce_wait(n, c)
            update_ref[rows(c)] = update_ref[rows(c)] + arrived[n, rows(c)]

    half = n // 2
    gather_send_hop(0, 0)
    for which in range(2):
        row_copy(which, 0).start()
        row_copy(which, 1).start()
    forward(0, 0)
    forward(1, 0)
    gather_send_hop(0, 1)
    forward(0, 1)
    row_wait(0, 0)
    row_copy(0, 2).start()
    forward(1, 1)
    gather_send_hop(0, 2)
    row_wait(0, 1)
    row_wait(0, 2)
    row_wait(1, 1)
    gather_wait(2, 0)
    compute_y(0)
    start_partials(0, 0, half)
    forward(0, 2)
    pass_on(1, 0, 0, half)
    forward(1, 2)
    gather_send_hop(0, 3)
    gather_wait(2, 1)
    compute_y(1)
    start_partials(1, 0, half)
    pass_on(2, 0, 0, half)
    row_wait(1, 0)
    row_copy(1, 2).start()
    pass_on(1, 1, 0, half)
    row_wait(1, 2)
    start_partials(0, half, n)
    start_partials(1, half, n)
    forward(0, 3)
    pass_on(2, 1, 0, half)
    pass_on(1, 0, half, n)
    forward(1, 3)
    pass_on(1, 1, half, n)
    gather_wait(2, 2)
    compute_y(2)
    start_partials(2, 0, n)
    pass_on(2, 0, half, n)
    pass_on(2, 1, half, n)
    compute_square(0)
    pass_on(1, 2, 0, n)
    gather_wait(2, 3)
    compute_y(3)
    start_partials(3, 0, n)
    pass_on(2, 2, 0, n)
    compute_square(1)
    pass_on(1, 3, 0, n)
    compute_square(2)
    pass_on(2, 3, 0, n)
    compute_square(3)
    for c in range(CHUNKS):
        finish(c)

    for which in range(2):
        for kind in range(3):
            row_copy(which, kind).wait_send()
    for c in range(CHUNKS):
        for hop in range(n - 1):
            gather_each(hop, c, lambda copy: copy.wait_send())

        def wait_sent(d, carry):
            @pl.when(d != z)
            def _():
                reduce_copy(LEFT, d, d, c).wait_send()

            return carry

        lax.fori_loop(0, n, wait_sent, 0)


def per_device(n, transition, covariance):
    size = transition.shape[0]
    f32 = jnp.float32
    shape = jax.ShapeDtypeStruct(transition.shape, f32)
    return pl.pallas_call(
        functools.partial(kernel, n),
        out_shape=(shape, shape),
        in_specs=[pl.BlockSpec(memory_space=pl.ANY)] * 2,
        out_specs=(pl.BlockSpec(memory_space=pltpu.VMEM),) * 2,
        scratch_shapes=[
            pltpu.VMEM((n, size, size), f32),
            pltpu.VMEM((n, size, size), f32),
            pltpu.VMEM((n, size, size), f32),
            pltpu.VMEM((n, size, size), f32),
            pltpu.VMEM((n + 1, size, size), f32),
            pltpu.VMEM((size, size), jnp.bfloat16),
            pltpu.VMEM((size, size), jnp.bfloat16),
            pltpu.SemaphoreType.DMA((3,)),
            pltpu.SemaphoreType.DMA((2, 3)),
            pltpu.SemaphoreType.DMA((2, 3)),
            pltpu.SemaphoreType.DMA((2, n - 1, CHUNKS)),
            pltpu.SemaphoreType.DMA((2, n - 1, CHUNKS)),
            pltpu.SemaphoreType.DMA((n, CHUNKS)),
            pltpu.SemaphoreType.DMA((n + 1, CHUNKS)),
        ],
        compiler_params=pltpu.CompilerParams(
            collective_id=0, has_side_effects=True, vmem_limit_bytes=67043328
        ),
    )(transition, covariance)


def solution(mesh):
    n = mesh.shape["col"]
    assert mesh.shape["row"] == n == 4
    spec = P(("eq", "row"), "col")
    return jax.shard_map(
        functools.partial(per_device, n),
        mesh=mesh,
        in_specs=(spec, spec),
        out_specs=(spec, spec),
        check_vma=False,
    )
```
